32 devices in a mesh: box: 4 (over z), tile: 8 (over y, x, core).
Axes of the slice: x: 2, y: 2, z: 4, core: 2. Of those that a mesh axis runs over, the one named last changes fastest.
Arguments:
- box_maps: float32 [4, 6, 448, 2688], P('box', None, 'tile'), may hold values from -4.01 to 4.01, as said below
- face_slots: int32 [4, 6], replicated, may hold values from 0 to 5, each once within a row
Outputs:
- final_map: float32 [7168, 7168], P('tile', 'box')
The draws below stay inside these ranges and needn't reach their ends.
Inputs may be any that keep to these rules, and one draw needn't show every extreme that they name: `box_maps`: read as a matrix of order 6 * 448 with rows and columns ordered by stored block and node, each box's map is exactly symmetric and positive definite. `face_slots`: each row is a permutation of the six stored blocks.
All inputs are finite; a program needn't handle non-finite values.
Results may differ from the reference program's by a relative error of at most 0.0001.
Values sent between devices are 32-bit elements; how exact they have to be, the bound alone decides.
A program may use at most 128 MiB of HBM per device.

```python
import math
import jax
import jax.numpy as jnp
from jax import lax

F = 448


def draw_box_maps(key, part):
    extent = 6 * F
    factor_key, weight_key = jax.random.split(jax.random.fold_in(key, 11), 2)
    factors = jax.random.truncated_normal(factor_key, -3.0, 3.0, (4, extent, extent), jnp.float32)
    weights = jnp.exp(jax.random.uniform(weight_key, (4, 1, extent), jnp.float32, math.log(0.05), math.log(5.0)))
    gramian = jnp.einsum('bik,bjk->bij', factors * weights, factors, precision=lax.Precision.HIGHEST) / extent
    matrices = gramian + 0.1 * jnp.eye(extent, dtype=jnp.float32)
    largest = jnp.max(jnp.diagonal(matrices, 0, 1, 2), axis=1)
    matrices = matrices * (4.0 / largest)[:, None, None]
    matrices = (matrices + jnp.swapaxes(matrices, 1, 2)) * 0.5
    return matrices.reshape(4, 6, F, extent)


def setup_inputs(seed: int = 0) -> dict:
    keys = jax.random.split(jax.random.key(seed), 3)
    return {
        "box_maps": draw_box_maps(jax.random.fold_in(keys[2], 71), 0),
        "face_slots": jax.vmap(lambda own: jax.random.permutation(own, 6))(jax.random.split(keys[1], 4)).reshape((4, 6)).astype(jnp.int32),
    }


def matmul(left, right):
    return jnp.dot(left.astype(jnp.float32), right.astype(jnp.float32), precision=lax.Precision.HIGHEST, preferred_element_type=jnp.float32)

def lower_solve(factor, coupled):
    return jax.scipy.linalg.solve_triangular(factor, coupled.T, lower=True).T

def reference(box_maps, face_slots):
    matrices = box_maps.reshape(4, 6 * F, 6 * F)

    def face_block(box_id, row_face, col_face):
        row_start = (face_slots[box_id, row_face] * F).astype(jnp.int32)
        col_start = (face_slots[box_id, col_face] * F).astype(jnp.int32)
        return lax.dynamic_slice(matrices[box_id], (row_start, col_start), (F, F))
    layouts = []
    for box_id in range(4):
        along_x, along_y = (box_id % 2, box_id // 2)
        layouts.append((1 - along_x, [along_x, 2 + along_y, 4, 5], 3 - along_y))
    level_one = []
    for pair_id in range(2):
        left_box, right_box = (2 * pair_id, 2 * pair_id + 1)
        summed = face_block(left_box, layouts[left_box][0], layouts[left_box][0]) + face_block(right_box, layouts[right_box][0], layouts[right_box][0])
        factor = jnp.linalg.cholesky(summed)
        for box_id in (left_box, right_box):
            x_shared, finals, y_shared = layouts[box_id]
            coupled = jnp.concatenate([face_block(box_id, surface, x_shared) for surface in finals + [y_shared]], 0)
            level_one.append(lower_solve(factor, coupled))
    zero_block = jnp.zeros((F, F), jnp.float32)
    pair_terms = []
    shared_rows = []
    for pair_id in range(2):
        left_box, right_box = (2 * pair_id, 2 * pair_id + 1)
        stacked = jnp.concatenate([level_one[left_box][4 * F:], level_one[right_box][4 * F:]], 0)
        shared_rows.append(stacked)
        left_face = face_block(left_box, layouts[left_box][2], layouts[left_box][2])
        right_face = face_block(right_box, layouts[right_box][2], layouts[right_box][2])
        diagonal = jnp.concatenate([jnp.concatenate([left_face, zero_block], 1), jnp.concatenate([zero_block, right_face], 1)], 0)
        pair_terms.append(diagonal - matmul(stacked, stacked.T))
    factor_two = jnp.linalg.cholesky(pair_terms[0] + pair_terms[1])
    level_two = []
    for box_id in range(4):
        x_shared, finals, y_shared = layouts[box_id]
        direct = jnp.concatenate([face_block(box_id, surface, y_shared) for surface in finals], 0)
        empty_part = jnp.zeros_like(direct)
        placed = jnp.concatenate([direct, empty_part] if box_id % 2 == 0 else [empty_part, direct], 1)
        coupled = placed - matmul(level_one[box_id][:4 * F], shared_rows[box_id // 2].T)
        level_two.append(lower_solve(factor_two, coupled))
    row_blocks = []
    for box_id in range(4):
        finals = layouts[box_id][1]
        entries = []
        for column_box in range(4):
            entry_block = jnp.zeros((4 * F, 4 * F), jnp.float32)
            if column_box == box_id:
                entry_block = entry_block + jnp.concatenate([jnp.concatenate([face_block(box_id, surface, other_face) for other_face in finals], 1) for surface in finals], 0)
            if column_box // 2 == box_id // 2:
                entry_block = entry_block - matmul(level_one[box_id][:4 * F], level_one[column_box][:4 * F].T)
            entry_block = entry_block - matmul(level_two[box_id], level_two[column_box].T)
            entries.append(entry_block)
        row_blocks.append(jnp.concatenate(entries, 1))
    return jnp.concatenate(row_blocks, 0)
```

```python
import jax
import jax.numpy as jnp
from jax import lax
from jax.experimental import pallas as pl
from jax.experimental.pallas import tpu as pltpu
from jax.sharding import PartitionSpec as P

F = 448


def partner(value, axis, bit):
    mask = 2**bit
    pairs = [(source, source ^ mask) for source in range(lax.axis_size(axis))]
    return lax.ppermute(value, axis, pairs)


def matmul(left, right):
    return jnp.dot(left, right, precision=lax.Precision.HIGHEST, preferred_element_type=jnp.float32)


BLOCK = 64


def eliminate(work_ref):
    size = work_ref.shape[0]

    def octet(index, carry):
        base = pl.multiple_of(index * 8, 8)
        whole = work_ref[...]
        panel = work_ref[pl.ds(base, 8), :]
        lanes = lax.broadcasted_iota(jnp.int32, whole.shape, 1)
        rows = lax.broadcasted_iota(jnp.int32, whole.shape, 0)
        panel_lanes = lax.broadcasted_iota(jnp.int32, panel.shape, 1)
        panel_rows = lax.broadcasted_iota(jnp.int32, panel.shape, 0)
        cols = [
            jnp.broadcast_to(jnp.sum(jnp.where(lanes == base + j, whole, 0.0), 1, keepdims=True), whole.shape)
            for j in range(8)
        ]
        pivots = [
            jnp.broadcast_to(
                jnp.sum(jnp.where(panel_lanes == base + j, panel, 0.0), 1, keepdims=True), panel.shape
            )
            for j in range(8)
        ]
        change = jnp.zeros_like(whole)
        for j in range(8):
            inverse = 1.0 / pivots[j][j : j + 1]
            below = jnp.where(panel_rows > j, pivots[j] * inverse, 0.0)
            scaled = cols[j] * inverse
            for k in range(j + 1, 8):
                head = pivots[k][j : j + 1]
                pivots[k] = pivots[k] - below * head
                cols[k] = cols[k] - scaled * head
            row = panel[j : j + 1]
            change = change + scaled * row
            panel = panel - below * row
        work_ref[...] = jnp.where(rows >= base + 8, whole - change, whole)
        work_ref[pl.ds(base, 8), :] = panel
        return carry

    lax.fori_loop(0, size // 8, octet, 0)
    done = work_ref[...]
    lanes = lax.broadcasted_iota(jnp.int32, done.shape, 1)
    rows = lax.broadcasted_iota(jnp.int32, done.shape, 0)
    diagonal = jnp.sum(jnp.where(lanes == rows, done, 0.0), 1, keepdims=True)
    return done[:, size:] * (1.0 / jnp.sqrt(diagonal))


def inverse_kernel(matrix_ref, out_ref, work_ref):
    order = matrix_ref.shape[0]
    out_ref[...] = matrix_ref[...]
    row_ids = lax.broadcasted_iota(jnp.int32, (BLOCK, BLOCK), 0)
    col_ids = lax.broadcasted_iota(jnp.int32, (BLOCK, BLOCK), 1)
    eye = jnp.where(row_ids == col_ids, 1.0, 0.0).astype(jnp.float32)
    for start in range(0, order, BLOCK):
        stop = start + BLOCK
        work_ref[...] = jnp.concatenate([out_ref[start:stop, start:stop], eye], 1)
        inverse = eliminate(work_ref)
        out_ref[start:, start:stop] = jnp.zeros((order - start, BLOCK), jnp.float32)
        out_ref[start:stop, start:stop] = eye
        panel = jnp.dot(
            inverse, out_ref[start:stop, :], precision=lax.Precision.HIGHEST, preferred_element_type=jnp.float32
        )
        if stop < order:
            left = panel[:, stop:].T
            for low in range(stop, order, BLOCK):
                piece = left[low - stop : low - stop + BLOCK]
                out_ref[low : low + BLOCK, :] -= jnp.dot(
                    piece, panel, precision=lax.Precision.HIGHEST, preferred_element_type=jnp.float32
                )
        lanes = lax.broadcasted_iota(jnp.int32, panel.shape, 1)
        out_ref[start:stop, :] = jnp.where(lanes < stop, panel, 0.0)


def inverse_factor(matrix):
    order = matrix.shape[0]
    return pl.pallas_call(
        inverse_kernel,
        out_shape=jax.ShapeDtypeStruct((order, order), jnp.float32),
        in_specs=[pl.BlockSpec(memory_space=pltpu.VMEM)],
        out_specs=pl.BlockSpec(memory_space=pltpu.VMEM),
        scratch_shapes=[pltpu.VMEM((BLOCK, 2 * BLOCK), jnp.float32)],
        cost_estimate=pl.CostEstimate(flops=100000000 * order, bytes_accessed=8 * order * order, transcendentals=0),
        compiler_params=pltpu.CompilerParams(vmem_limit_bytes=40 * 2**20),
        name="inverse_factor",
    )(matrix)


def face_columns(stored, slot_id):
    return lax.dynamic_slice_in_dim(stored, slot_id * F, F, stored.ndim - 1)


def beside(block_part, leading):
    empty_part = jnp.zeros_like(block_part)
    return jnp.where(
        leading,
        jnp.concatenate([block_part, empty_part], -1),
        jnp.concatenate([empty_part, block_part], -1),
    )


def ordered(own_piece, theirs, leading, axis_id):
    return jnp.where(
        leading,
        jnp.concatenate([own_piece, theirs], axis_id),
        jnp.concatenate([theirs, own_piece], axis_id),
    )


def per_device(box_maps, face_slots):
    stored = box_maps[0]
    node_count = stored.shape[1]
    box_id = lax.axis_index("box")
    along_x = box_id % 2
    along_y = box_id // 2
    leading = along_x == 0
    slot_row = lax.dynamic_index_in_dim(face_slots, box_id, 0, keepdims=False)

    def slot_of(surface):
        return lax.dynamic_index_in_dim(slot_row, surface, 0, keepdims=False)

    x_shared = slot_of(1 - along_x)
    y_shared = slot_of(3 - along_y)
    finals = [slot_of(along_x), slot_of(2 + along_y), slot_row[4], slot_row[5]]
    outer_rows = jnp.stack(
        [
            lax.dynamic_index_in_dim(stored, slot_id, 0, keepdims=False)
            for slot_id in finals + [y_shared]
        ]
    )
    shared_face = lax.dynamic_index_in_dim(stored, x_shared, 0, keepdims=False)
    own_part = face_columns(shared_face, x_shared)
    summed = own_part + partner(own_part, "box", 0)
    inverse_one = inverse_factor(lax.all_gather(summed, "tile", axis=0, tiled=True))
    level_one = matmul(
        face_columns(outer_rows, x_shared).reshape(5 * node_count, F), inverse_one.T
    ).reshape(5, node_count, F)
    final_one = level_one[:4].reshape(4 * node_count, F)
    pairing_rows = level_one[4]
    partner_rows = partner(pairing_rows, "box", 0)
    pair_rows = lax.all_gather(
        ordered(pairing_rows[None], partner_rows[None], leading, 0), "tile", axis=1, tiled=True
    ).reshape(2 * F, F)
    partial_rows = beside(face_columns(outer_rows[4], y_shared), leading) - matmul(
        pairing_rows, pair_rows.T
    )
    summed_rows = partial_rows + partner(partial_rows, "box", 1)
    half_rows = lax.all_gather(summed_rows, "tile", axis=0, tiled=True)
    shared_two = ordered(half_rows, partner(half_rows, "box", 0), leading, 0)
    inverse_two = inverse_factor(shared_two)
    coupled = beside(face_columns(outer_rows[:4], y_shared), leading).reshape(
        4 * node_count, 2 * F
    ) - matmul(final_one, pair_rows.T)
    level_two = matmul(coupled, inverse_two.T)
    own_block = jnp.concatenate([face_columns(outer_rows[:4], slot_id) for slot_id in finals], 2)
    tile_count = lax.axis_size("tile")
    tile_bits = tile_count.bit_length() - 1
    column_bits = (tile_bits + 1) // 2
    columns = 1 << column_bits
    high_count = tile_count >> column_bits
    tile_id = lax.axis_index("tile")
    group_rows = 4 * columns * node_count
    box_span = 4 * high_count * node_count

    def panel_of(piece):
        for bit_id in range(column_bits):
            lower_half = (tile_id >> bit_id) % 2 == 0
            piece = ordered(piece, partner(piece, "tile", bit_id), lower_half, 1)
        return piece.reshape(group_rows, piece.shape[-1])

    def columns_of(piece):
        piece = piece[:, None]
        for bit_id in range(column_bits, tile_bits):
            lower_half = (tile_id >> bit_id) % 2 == 0
            piece = ordered(piece, partner(piece, "tile", bit_id), lower_half, 1)
        return piece

    first_rows = final_one.reshape(4, node_count, F)
    second_rows = level_two.reshape(4, node_count, 2 * F)
    column_own = columns_of(own_block)
    first_cols = columns_of(first_rows).reshape(1, box_span, F)
    pair_cols = ordered(first_cols, partner(first_cols, "box", 0), leading, 0).reshape(2 * box_span, F)
    column_rows = lax.all_gather(columns_of(second_rows), "box", axis=0, tiled=True).reshape(
        4 * box_span, 2 * F
    )
    pair_id = box_id // 2
    pair_term = matmul(panel_of(first_rows), pair_cols.T)
    group_id = tile_id >> column_bits
    mirrored = lax.dynamic_slice_in_dim(
        column_own.reshape(4, high_count, node_count, 4, F),
        group_id * columns * node_count,
        columns * node_count,
        4,
    )
    own_term = mirrored.transpose(3, 4, 0, 1, 2).reshape(group_rows, box_span)
    own_cols = lax.dynamic_slice_in_dim(pair_term, along_x * box_span, box_span, 1)
    pair_block = lax.dynamic_update_slice_in_dim(
        -pair_term, own_term - own_cols, along_x * box_span, 1
    )
    level_block = lax.dynamic_update_slice_in_dim(
        jnp.zeros((group_rows, 4 * box_span), jnp.float32), pair_block, pair_id * 2 * box_span, 1
    )
    level_block = level_block - matmul(panel_of(second_rows), column_rows.T)
    piece_width = 16 * node_count // columns
    outgoing = level_block.reshape(group_rows, tile_count, piece_width)
    incoming = lax.all_to_all(outgoing, "tile", split_axis=1, concat_axis=1, tiled=True)
    incoming = incoming.reshape(
        4, columns * node_count, high_count, columns, 16 // columns, node_count
    )
    return incoming.transpose(4, 3, 5, 0, 2, 1).reshape(16 * node_count, 4 * F)


def solution(mesh):
    return jax.shard_map(
        per_device,
        mesh=mesh,
        in_specs=(P("box", None, "tile", None), P()),
        out_specs=P("tile", "box"),
        check_vma=False,
    )
```
